8 devices in a mesh: dp: 1 (over z), sp: 8 (over y, x, core).
Axes of the slice: x: 2, y: 2, z: 1, core: 2. Of those that a mesh axis runs over, the one named last changes fastest.
Arguments:
- x_in: bfloat16 [4, 2048, 2048], P('dp', 'sp')
- positions: int32 [4, 2048], P('dp', 'sp')
- keep_mask: int32 [4, 2048], P('dp', 'sp')
- ln_gain: float32 [2048], replicated
- ln_bias: float32 [2048], replicated
- w_qkv: bfloat16 [2048, 16, 3, 128], replicated
- b_qkv: float32 [16, 3, 128], replicated
- w_out: bfloat16 [2048, 2048], replicated
- b_out: float32 [2048], replicated
- grad_y: bfloat16 [4, 2048, 2048], P('dp', 'sp')
Outputs:
- output 1: bfloat16 [4, 2048, 2048], P('dp', 'sp')
- output 2: bfloat16 [4, 2048, 2048], P('dp', 'sp')
- output 3: float32 [2048, 16, 3, 128], P('dp')
- output 4: float32 [16, 3, 128], P('dp')
- output 5: float32 [2048, 2048], P('dp')
- output 6: float32 [2048], P('dp')
- output 7: float32 [2048], P('dp')
- output 8: float32 [2048], P('dp')
All inputs are finite; a program needn't handle non-finite values.
Results may differ from the reference program's by a relative error of at most 0.00988608.
Values are sent between devices in bfloat16 or wider.
A program may use at most 1 GiB of HBM per device.

```python
import jax
import jax.numpy as jnp
import numpy as np
from jax import lax

BATCH_SEQS = 4
SEQ_LEN = 2048
HIDDEN = 2048
NUM_HEADS = 16
HEAD_DIM = HIDDEN // NUM_HEADS
NORM_EPS = 1e-5
MASK_FILL = -1e30
QK_SCALE = HEAD_DIM ** -0.5
SLOPES = 2.0 ** (-8.0 * (np.arange(NUM_HEADS) + 1) / NUM_HEADS)


def setup_inputs(seed: int = 0, part: int = 0) -> dict:
    part_key = jax.random.fold_in(jax.random.key(seed), part)
    k_x, k_dy, k_len, k_gap = jax.random.split(part_key, 4)
    k_g, k_b, k_wq, k_bq, k_wo, k_bo = jax.random.split(jax.random.key(seed + 1), 6)
    shape_act = (BATCH_SEQS, SEQ_LEN, HIDDEN)
    x_in = jax.random.normal(k_x, shape_act, jnp.float32).astype(jnp.bfloat16)
    grad_y = jax.random.normal(k_dy, shape_act, jnp.float32).astype(jnp.bfloat16)
    lengths = jax.random.randint(k_len, (BATCH_SEQS,), SEQ_LEN // 8, SEQ_LEN + 1)
    lengths = lengths.at[0].set(SEQ_LEN)
    keep_mask = (jnp.arange(SEQ_LEN)[None, :] < lengths[:, None]).astype(jnp.int32)
    pos_steps = jax.random.randint(k_gap, (BATCH_SEQS, SEQ_LEN), 1, 3)
    positions = (jnp.cumsum(pos_steps, axis=1) - pos_steps[:, :1]).astype(jnp.int32)
    w_scale = HIDDEN ** -0.5
    return {
        "x_in": x_in,
        "positions": positions,
        "keep_mask": keep_mask,
        "ln_gain": 1.0 + 0.5 * jax.random.normal(k_g, (HIDDEN,), jnp.float32),
        "ln_bias": 0.5 * jax.random.normal(k_b, (HIDDEN,), jnp.float32),
        "w_qkv": (w_scale * jax.random.normal(k_wq, (HIDDEN, NUM_HEADS, 3, HEAD_DIM), jnp.float32)).astype(jnp.bfloat16),
        "b_qkv": 0.5 * jax.random.normal(k_bq, (NUM_HEADS, 3, HEAD_DIM), jnp.float32),
        "w_out": (w_scale * jax.random.normal(k_wo, (HIDDEN, HIDDEN), jnp.float32)).astype(jnp.bfloat16),
        "b_out": 0.5 * jax.random.normal(k_bo, (HIDDEN,), jnp.float32),
        "grad_y": grad_y,
    }


def head_probs(q_head, k_head, pos_row, keep_row, head_slope):
    scores = jnp.dot(q_head, k_head.T, preferred_element_type=jnp.float32) * QK_SCALE
    pos_gap = (pos_row[:, None] - pos_row[None, :]).astype(jnp.float32)
    scores = scores - head_slope * pos_gap
    tok_index = jnp.arange(SEQ_LEN)
    allowed = (tok_index[None, :] <= tok_index[:, None]) & (keep_row[None, :] > 0)
    return jax.nn.softmax(jnp.where(allowed, scores, MASK_FILL), axis=-1)


def head_forward(head_item):
    q_head, k_head, v_head, pos_row, keep_row, head_slope = head_item
    attn_prob = head_probs(q_head, k_head, pos_row, keep_row, head_slope)
    return jnp.dot(attn_prob.astype(jnp.bfloat16), v_head, preferred_element_type=jnp.float32).astype(jnp.bfloat16)


def head_backward(head_item):
    q_head, k_head, v_head, o_head, do_head, pos_row, keep_row, head_slope = head_item
    attn_prob = head_probs(q_head, k_head, pos_row, keep_row, head_slope)
    prob_lo = attn_prob.astype(jnp.bfloat16)
    dv_head = jnp.dot(prob_lo.T, do_head, preferred_element_type=jnp.float32).astype(jnp.bfloat16)
    grad_prob = jnp.dot(do_head, v_head.T, preferred_element_type=jnp.float32)
    row_dot = jnp.sum(do_head.astype(jnp.float32) * o_head.astype(jnp.float32), axis=-1)
    ds_lo = (attn_prob * (grad_prob - row_dot[:, None])).astype(jnp.bfloat16)
    dq_head = (jnp.dot(ds_lo, k_head, preferred_element_type=jnp.float32) * QK_SCALE).astype(jnp.bfloat16)
    dk_head = (jnp.dot(ds_lo.T, q_head, preferred_element_type=jnp.float32) * QK_SCALE).astype(jnp.bfloat16)
    return dq_head, dk_head, dv_head


def reference(x_in, positions, keep_mask, ln_gain, ln_bias, w_qkv, b_qkv, w_out, b_out, grad_y):
    tokens = BATCH_SEQS * SEQ_LEN
    x_f32 = x_in.astype(jnp.float32)
    centered = x_f32 - jnp.mean(x_f32, axis=-1, keepdims=True)
    inv_std = lax.rsqrt(jnp.mean(centered * centered, axis=-1, keepdims=True) + NORM_EPS)
    x_hat = centered * inv_std
    x_norm = (x_hat * ln_gain + ln_bias).astype(jnp.bfloat16).reshape(tokens, HIDDEN)
    w_flat = w_qkv.reshape(HIDDEN, 3 * HIDDEN)
    qkv_flat = (jnp.dot(x_norm, w_flat, preferred_element_type=jnp.float32) + b_qkv.reshape(3 * HIDDEN)).astype(jnp.bfloat16)
    qkv_heads = jnp.transpose(qkv_flat.reshape(BATCH_SEQS, SEQ_LEN, NUM_HEADS, 3, HEAD_DIM), (3, 0, 2, 1, 4))
    qkv_heads = qkv_heads.reshape(3, BATCH_SEQS * NUM_HEADS, SEQ_LEN, HEAD_DIM)
    pos_rows = jnp.repeat(positions, NUM_HEADS, axis=0)
    keep_rows = jnp.repeat(keep_mask, NUM_HEADS, axis=0)
    slope_rows = jnp.tile(jnp.asarray(SLOPES, jnp.float32), BATCH_SEQS)
    o_heads = lax.map(head_forward, (qkv_heads[0], qkv_heads[1], qkv_heads[2], pos_rows, keep_rows, slope_rows))
    o_flat = jnp.transpose(o_heads.reshape(BATCH_SEQS, NUM_HEADS, SEQ_LEN, HEAD_DIM), (0, 2, 1, 3)).reshape(tokens, HIDDEN)
    y_out = (x_f32.reshape(tokens, HIDDEN) + jnp.dot(o_flat, w_out, preferred_element_type=jnp.float32) + b_out).astype(jnp.bfloat16)
    dy_flat = grad_y.reshape(tokens, HIDDEN)
    grad_b_out = jnp.sum(dy_flat.astype(jnp.float32), axis=0)
    grad_w_out = jnp.dot(o_flat.T, dy_flat, preferred_element_type=jnp.float32)
    do_flat = jnp.dot(dy_flat, w_out.T, preferred_element_type=jnp.float32).astype(jnp.bfloat16)
    do_heads = jnp.transpose(do_flat.reshape(BATCH_SEQS, SEQ_LEN, NUM_HEADS, HEAD_DIM), (0, 2, 1, 3)).reshape(BATCH_SEQS * NUM_HEADS, SEQ_LEN, HEAD_DIM)
    dq_heads, dk_heads, dv_heads = lax.map(head_backward, (qkv_heads[0], qkv_heads[1], qkv_heads[2], o_heads, do_heads, pos_rows, keep_rows, slope_rows))
    d_qkv = jnp.stack([dq_heads, dk_heads, dv_heads], axis=0).reshape(3, BATCH_SEQS, NUM_HEADS, SEQ_LEN, HEAD_DIM)
    d_qkv = jnp.transpose(d_qkv, (1, 3, 2, 0, 4)).reshape(tokens, 3 * HIDDEN)
    grad_b_qkv = jnp.sum(d_qkv.astype(jnp.float32), axis=0).reshape(NUM_HEADS, 3, HEAD_DIM)
    grad_w_qkv = jnp.dot(x_norm.T, d_qkv, preferred_element_type=jnp.float32).reshape(HIDDEN, NUM_HEADS, 3, HEAD_DIM)
    d_norm = jnp.dot(d_qkv, w_flat.T, preferred_element_type=jnp.float32).reshape(BATCH_SEQS, SEQ_LEN, HIDDEN)
    grad_gain = jnp.sum(d_norm * x_hat, axis=(0, 1))
    grad_bias = jnp.sum(d_norm, axis=(0, 1))
    d_hat = d_norm * ln_gain
    d_ln = inv_std * (d_hat - jnp.mean(d_hat, axis=-1, keepdims=True) - x_hat * jnp.mean(d_hat * x_hat, axis=-1, keepdims=True))
    grad_x = (grad_y.astype(jnp.float32) + d_ln).astype(jnp.bfloat16)
    return (y_out.reshape(BATCH_SEQS, SEQ_LEN, HIDDEN), grad_x, grad_w_qkv, grad_b_qkv, grad_w_out, grad_b_out, grad_gain, grad_bias)
```

```python
import functools

import jax
import jax.numpy as jnp
from jax import lax
from jax.experimental import pallas as pl
from jax.experimental.pallas import tpu as pltpu
from jax.sharding import PartitionSpec as P


NORM_EPS = 1e-5
MASK_FILL = -1e30
LOG2E = 1.4426950408889634


NT = (((1,), (1,)), ((), ()))
NN = (((1,), (0,)), ((), ()))


def dot(a, b, dims=NN):
    return lax.dot_general(a, b, dims, preferred_element_type=jnp.float32)


def stage_kernel(me_ref, slope_ref, x0_ref, x1_ref, d0_ref, d1_ref, w_ref, b_ref, wo_ref, pos_ref, *refs, nblk, blk, dim, heads, scale, first):
    if first:
        gwi_ref = gwoi_ref = None
    else:
        gwi_ref, gwoi_ref = refs[:2]
        refs = refs[2:]
    out_ref, gw_ref, gwo_ref, qkv_ref, do_ref, s_ref, dk_ref, dv_ref, kt_ref, vt_ref, ot_ref, dqp_ref, xv_ref, dv_all_ref, x_sem, d_sem = refs
    step = pl.program_id(0)
    me = me_ref[0]
    width = 3 * dim
    half = nblk // 2

    def load(b):
        p, at = b // half, pl.ds((b % half) * blk, blk)
        return (pltpu.make_async_copy((x0_ref, x1_ref)[p].at[at], xv_ref.at[b], x_sem.at[b]),
                pltpu.make_async_copy((d0_ref, d1_ref)[p].at[at], dv_all_ref.at[b], d_sem.at[b]))

    @pl.when(step == 0)
    def _():
        for b in range(nblk):
            for copy in load(b):
                copy.start()

    for b in range(nblk):
        @pl.when(step == b)
        def _(b=b):
            for copy in load(b):
                copy.wait()

    @pl.when(step < nblk)
    def _():
        at = pl.ds(pl.multiple_of(step * blk, blk), blk)
        qkv = (dot(xv_ref[step], w_ref[...]) + b_ref[...]).astype(jnp.bfloat16)
        qkv_ref[at, :] = qkv
        do_ref[at, :] = dot(dv_all_ref[step], wo_ref[...], NT).astype(jnp.bfloat16)
        for h in range(heads):
            kt_ref[h, step] = qkv[:, h * width + dim:h * width + 2 * dim].T
            vt_ref[h, step] = qkv[:, h * width + 2 * dim:(h + 1) * width].T

    @pl.when(step == 0)
    def _():
        dk_ref[...] = jnp.zeros_like(dk_ref)
        dv_ref[...] = jnp.zeros_like(dv_ref)

    @pl.when((step >= nblk) & (step < 2 * nblk))
    def _():
        attend(step - nblk, me, slope_ref, qkv_ref, do_ref, pos_ref, out_ref, s_ref, dk_ref, dv_ref, kt_ref, vt_ref, ot_ref, dqp_ref,
               nblk=nblk, blk=blk, dim=dim, heads=heads, scale=scale)

    @pl.when(step >= 2 * nblk)
    def _():
        tile = gw_ref.shape[0]
        cols = pl.ds(pl.multiple_of((step - 2 * nblk) * tile, tile), tile)
        xt = jnp.concatenate([xv_ref[b, :, cols] for b in range(nblk)], axis=0)
        gw = dot(xt.T, dqp_ref[...])
        gwo = 0.0
        for b in range(nblk):
            gwo += dot(ot_ref[b], dv_all_ref[b, :, cols])
        gw_ref[...] = gw if first else gwi_ref[...] + gw
        gwo_ref[...] = gwo if first else gwoi_ref[...] + gwo


def attend(i, me, slope_ref, qkv_ref, do_ref, pos_ref, out_ref, s_ref, dk_ref, dv_ref, kt_ref, vt_ref, ot_ref, dqp_ref,
           *, nblk, blk, dim, heads, scale):
    width = 3 * dim

    def block_of(j):
        r = jnp.bitwise_xor(j, me)
        return lax.rem(r, 2) * (nblk // 2) + lax.div(r, 2)

    def rows(j):
        return pl.ds(pl.multiple_of(block_of(j) * blk, blk), blk)

    def fold(t, op):
        return op(t.reshape(blk // 8, 8, blk), axis=0)

    qrows = rows(i)
    orows = pl.ds(pl.multiple_of(i * blk, blk), blk)
    qs = [qkv_ref[qrows, h * width:h * width + dim] for h in range(heads)]
    dos = [do_ref[qrows, h * dim:(h + 1) * dim] for h in range(heads)]
    dots = [d.T for d in dos]
    pos_first = pos_ref[pl.ds(pl.multiple_of(i * blk, blk), 8), 0:1][:1]

    def scores(j, h):
        k = qkv_ref[rows(j), h * width + dim:h * width + 2 * dim]
        lrows = pl.ds(pl.multiple_of(j * blk, blk), blk)
        bias = (pos_ref[lrows, 0:1] - pos_first) * slope_ref[h] + pos_ref[lrows, 1:2]
        return dot(k, qs[h], NT) * (scale * LOG2E) + bias

    pairs = lax.div(i, 2)
    gap = lax.broadcasted_iota(jnp.int32, (blk, blk), 0) - lax.broadcasted_iota(jnp.int32, (blk, blk), 1)

    def score_pair(m, mx, masked):
        new = list(mx)
        for t in range(2):
            j = 2 * m + t
            for h in range(heads):
                s = scores(j, h)
                if masked:
                    s = jnp.where(gap <= (i - j) * blk, s, MASK_FILL)
                s_ref[h, j] = s
                new[h] = jnp.maximum(new[h], fold(s, jnp.max))
        return tuple(new)

    start = tuple(jnp.full((8, blk), MASK_FILL, jnp.float32) for _ in range(heads))
    mx = lax.fori_loop(0, pairs, lambda m, c: score_pair(m, c, False), start)
    mx = score_pair(pairs, mx, True)
    tops = [jnp.max(v, axis=0, keepdims=True) for v in mx]

    def weigh_pair(m, carry):
        tot, acc = list(carry[0]), list(carry[1])
        for t in range(2):
            j = 2 * m + t
            for h in range(heads):
                p = jnp.exp2(s_ref[h, j] - tops[h])
                s_ref[h, j] = p
                tot[h] = tot[h] + fold(p, jnp.sum)
                acc[h] = acc[h] + dot(vt_ref[h, block_of(j)], p.astype(jnp.bfloat16))
        return tuple(tot), tuple(acc)

    zero_t = tuple(jnp.zeros((dim, blk), jnp.float32) for _ in range(heads))
    tot, ots = lax.fori_loop(0, pairs + 1, weigh_pair, (tuple(jnp.zeros((8, blk), jnp.float32) for _ in range(heads)), zero_t))
    inv = [1.0 / jnp.sum(t, axis=0, keepdims=True) for t in tot]
    rs = []
    for h in range(heads):
        o_lo = (ots[h] * inv[h]).astype(jnp.bfloat16)
        rs.append(jnp.sum(dots[h].astype(jnp.float32) * o_lo.astype(jnp.float32), axis=0, keepdims=True))
        ot_ref[block_of(i), h * dim:(h + 1) * dim, :] = o_lo
        out_ref[orows, heads * width + h * dim:heads * width + (h + 1) * dim] = o_lo.T

    def grad_pair(m, acc):
        new = list(acc)
        for t in range(2):
            jx = block_of(2 * m + t)
            for h in range(heads):
                v = qkv_ref[rows(2 * m + t), h * width + 2 * dim:(h + 1) * width]
                p = s_ref[h, 2 * m + t] * inv[h]
                ds = (p * (dot(v, dos[h], NT) - rs[h])).astype(jnp.bfloat16)
                dv_ref[h, jx] += dot(p.astype(jnp.bfloat16), dos[h])
                dk_ref[h, jx] += dot(ds, qs[h])
                new[h] = new[h] + dot(kt_ref[h, jx], ds)
        return tuple(new)

    dqts = lax.fori_loop(0, pairs + 1, grad_pair, zero_t)
    for h in range(heads):
        dq = (dqts[h] * scale).astype(jnp.bfloat16).T
        out_ref[orows, h * width:h * width + dim] = dq
        dqp_ref[qrows, h * width:h * width + dim] = dq

    @pl.when(i == nblk - 1)
    def _():
        for b in range(nblk):
            r = 2 * (b % (nblk // 2)) + b // (nblk // 2)
            lrows = pl.ds(pl.multiple_of(jnp.bitwise_xor(me, r) * blk, blk), blk)
            for h in range(heads):
                dk = (dk_ref[h, b] * scale).astype(jnp.bfloat16)
                dv = dv_ref[h, b].astype(jnp.bfloat16)
                for ref, at in ((out_ref, lrows), (dqp_ref, slice(b * blk, (b + 1) * blk))):
                    ref[at, h * width + dim:h * width + 2 * dim] = dk
                    ref[at, h * width + 2 * dim:(h + 1) * width] = dv


def stage(me, slopes, x_two, d_two, w, b, wo, pos, gw, gwo, nblk, heads, dim):
    n, hidden = x_two[0].shape
    seq = 2 * n
    blk = seq // nblk
    width, owidth = 3 * heads * dim, heads * dim
    tile = hidden // nblk
    first = gw is None
    body = functools.partial(stage_kernel, nblk=nblk, blk=blk, dim=dim, heads=heads, scale=dim ** -0.5, first=first)
    tiles = heads * nblk * (nblk + 1) // 2

    def late(i):
        return jnp.maximum(i - 2 * nblk, 0)

    def fixed(shape):
        return pl.BlockSpec(shape, lambda i, m: (0, 0), pipeline_mode=pl.Buffered(1))

    gw_spec = pl.BlockSpec((tile, width), lambda i, m: (late(i), 0))
    gwo_spec = pl.BlockSpec((owidth, tile), lambda i, m: (0, late(i)))
    args = [x_two[0], x_two[1], d_two[0], d_two[1], w, b, wo, pos]
    in_specs = [pl.BlockSpec(memory_space=pltpu.SMEM)] + [pl.BlockSpec(memory_space=pl.ANY)] * 4 + [
                fixed(w.shape), fixed(b.shape), fixed(wo.shape), fixed(pos.shape)]
    aliases = {}
    if not first:
        args += [gw, gwo]
        in_specs += [gw_spec, gwo_spec]
        aliases = {10: 1, 11: 2}
    flops = tiles * 12 * blk * blk * dim + 4 * seq * hidden * (width + owidth)
    return pl.pallas_call(
        body,
        grid_spec=pltpu.PrefetchScalarGridSpec(
            num_scalar_prefetch=1,
            grid=(3 * nblk,),
            in_specs=in_specs,
            out_specs=[pl.BlockSpec((seq, width + owidth), lambda i, m: (0, 0), pipeline_mode=pl.Buffered(1)), gw_spec, gwo_spec],
            scratch_shapes=[
                pltpu.VMEM((seq, width), jnp.bfloat16),
                pltpu.VMEM((seq, owidth), jnp.bfloat16),
                pltpu.VMEM((heads, nblk, blk, blk), jnp.float32),
                pltpu.VMEM((heads, nblk, blk, dim), jnp.float32),
                pltpu.VMEM((heads, nblk, blk, dim), jnp.float32),
                pltpu.VMEM((heads, nblk, dim, blk), jnp.bfloat16),
                pltpu.VMEM((heads, nblk, dim, blk), jnp.bfloat16),
                pltpu.VMEM((nblk, owidth, blk), jnp.bfloat16),
                pltpu.VMEM((seq, width), jnp.bfloat16),
                pltpu.VMEM((nblk, blk, hidden), jnp.bfloat16),
                pltpu.VMEM((nblk, blk, hidden), jnp.bfloat16),
                pltpu.SemaphoreType.DMA((nblk,)),
                pltpu.SemaphoreType.DMA((nblk,)),
            ],
        ),
        out_shape=[jax.ShapeDtypeStruct((seq, width + owidth), jnp.bfloat16),
                   jax.ShapeDtypeStruct((hidden, width), jnp.float32),
                   jax.ShapeDtypeStruct((owidth, hidden), jnp.float32)],
        input_output_aliases=aliases,
        compiler_params=pltpu.CompilerParams(
            dimension_semantics=("arbitrary",), vmem_limit_bytes=60 * 1024 * 1024),
        cost_estimate=pl.CostEstimate(flops=flops, bytes_accessed=seq * hidden * 8, transcendentals=tiles * blk * blk),
        name="stage",
    )(me, slopes, *args)


def place_kernel(me_ref, p0, p1, p2, p3, *refs, heads, dim, group):
    out_ref = refs[-1]
    pieces = (p0, p1, p2, p3)
    mine = lax.rem(me_ref[0], group)
    for m in range(group):
        @pl.when(mine == m)
        def _(m=m):
            for r in range(group):
                for h in range(heads):
                    for c in range(3):
                        at = (h * 3 + c) * dim
                        out_ref[:, c, (m ^ r) * heads + h, :] = pieces[r][:, at:at + dim]


def place(me, pieces, far, row, full, shape, heads, dim):
    group = len(pieces)
    n, width = pieces[0].shape
    rows = 128
    first = row // rows
    aliases = {}
    args = list(pieces)
    in_specs = [pl.BlockSpec((rows, width), lambda g, m: (g, 0))] * group
    if full is not None:
        in_specs.append(pl.BlockSpec(memory_space=pl.ANY))
        args.append(full)
        aliases = {group + 1: 0}
    return pl.pallas_call(
        functools.partial(place_kernel, heads=heads, dim=dim, group=group),
        grid_spec=pltpu.PrefetchScalarGridSpec(
            num_scalar_prefetch=1,
            grid=(n // rows,),
            in_specs=in_specs,
            out_specs=pl.BlockSpec(
                (rows, 3, group * heads, dim),
                lambda g, m: (first + g, 0, jnp.bitwise_xor(lax.div(m[0], group), far), 0)),
        ),
        out_shape=jax.ShapeDtypeStruct(shape, jnp.float32),
        input_output_aliases=aliases,
        cost_estimate=pl.CostEstimate(flops=group * n * width * 30, bytes_accessed=group * n * width * 8, transcendentals=0),
        name="place",
    )(me, *args)


def stack_kernel(me_ref, *refs):
    out_ref = refs[-1]
    for r, p_ref in enumerate(refs[:-1]):
        out_ref[jnp.bitwise_xor(me_ref[0], r)] = p_ref[...]


def stack_rows(me, pieces):
    n, width = pieces[0].shape
    rows = 32
    return pl.pallas_call(
        stack_kernel,
        grid_spec=pltpu.PrefetchScalarGridSpec(
            num_scalar_prefetch=1,
            grid=(n // rows,),
            in_specs=[pl.BlockSpec((rows, width), lambda g, m: (g, 0))] * len(pieces),
            out_specs=pl.BlockSpec((len(pieces), rows, width), lambda g, m: (0, g, 0)),
        ),
        out_shape=jax.ShapeDtypeStruct((len(pieces), n, width), jnp.float32),
        cost_estimate=pl.CostEstimate(flops=len(pieces) * n * width * 4, bytes_accessed=len(pieces) * n * width * 8, transcendentals=0),
        name="stack_rows",
    )(me, *pieces)


CHUNKS = (640, 640, 512, 256)


def after(value, *others):
    return lax.optimization_barrier((value,) + others)[0]


def solution(mesh):
    sp_size = mesh.shape["sp"]

    def swap(v, r):
        return lax.ppermute(v, "sp", [(i, i ^ r) for i in range(sp_size)])

    def gather(b):
        half = b.shape[0] // 2
        bx, by, bs = swap(b, 2), swap(b, 4), swap(b, 1)
        bd = jnp.concatenate([swap(bx[:half], 4), swap(by[half:], 2)], 0)
        return [b, bs, bx, swap(bx, 1), by, swap(by, 1), bd, swap(bd, 1)]

    def gather_halves(b):
        half = b.shape[0] // 2
        bx, by = swap(b, 2), swap(b, 4)
        mine = jnp.concatenate([b, bx, by, swap(bx[:half], 4), swap(by[half:], 2)], 0)
        return mine, swap(mine, 1)

    def block_fn(x_blk, pos_blk, keep_blk, ln_gain, ln_bias, w_qkv, b_qkv, w_out, b_out, dy_blk):
        batch_loc, seq_loc, hidden = x_blk.shape
        num_heads, head_dim = w_qkv.shape[1], w_qkv.shape[3]
        heads = num_heads // sp_size
        width = heads * 3 * head_dim
        owidth = heads * head_dim
        me = lax.axis_index("sp")
        me_arr = me.reshape(1).astype(jnp.int32)

        def stats(x):
            x_f32 = x.astype(jnp.float32)
            centered = x_f32 - jnp.mean(x_f32, axis=-1, keepdims=True)
            inv_std = lax.rsqrt(jnp.mean(centered * centered, axis=-1, keepdims=True) + NORM_EPS)
            return x_f32, centered * inv_std, inv_std

        def norm(x):
            return (stats(x)[1] * ln_gain + ln_bias).astype(jnp.bfloat16)

        x_norms = [norm(x_blk[s]) for s in range(batch_loc)]

        pk = jnp.stack([pos_blk, keep_blk])
        pk_all = jnp.stack([pk] + [swap(pk, r) for r in range(1, sp_size)])
        pk_all = pk_all[jnp.arange(sp_size) ^ me]
        pk_all = jnp.transpose(pk_all, (1, 2, 0, 3)).reshape(2, batch_loc, sp_size * seq_loc)
        pos_col = jnp.stack([pk_all[0].astype(jnp.float32), jnp.where(pk_all[1] > 0, 0.0, MASK_FILL)], axis=-1)
        head_ids = me * heads + jnp.arange(heads)
        slopes = jnp.exp2(-8.0 * (head_ids + 1).astype(jnp.float32) / num_heads) * LOG2E

        w_flat = after(w_qkv, x_norms[0]).reshape(hidden, sp_size * width)
        w_mine = lax.dynamic_slice_in_dim(w_flat, me * width, width, 1)
        b_mine = lax.dynamic_slice_in_dim(b_qkv.reshape(sp_size, width), me, 1, 0)
        wo_mine = lax.dynamic_slice_in_dim(w_out, me * owidth, owidth, 0)

        gw = gwo = None
        results, parts = [], []
        for s in range(batch_loc):
            x_two = gather_halves(x_norms[s])
            d_two = gather_halves(dy_blk[s])
            res, gw, gwo = stage(me_arr, slopes, x_two, d_two, w_mine, b_mine, wo_mine, pos_col[s], gw, gwo,
                                 sp_size, heads, head_dim)
            parts.append(lax.all_to_all(res.reshape(sp_size, seq_loc, width + owidth), "sp", 0, 0, tiled=True))
            results.append(res)
        gb_mine = sum(jnp.sum(after(d, gw)[:, :width].astype(jnp.float32), axis=0) for d in results)

        got = jnp.stack(lax.optimization_barrier((parts, gw))[0])
        got = jnp.transpose(got, (0, 2, 1, 3))
        dq_loc = got[..., :width].reshape(batch_loc, seq_loc, sp_size * width)
        o_loc = got[..., width:].reshape(batch_loc, seq_loc, hidden)
        x_f32, x_hat, inv_std = stats(after(x_blk, gw))
        y_blk = (x_f32 + jnp.einsum("bsh,hk->bsk", o_loc, w_out, preferred_element_type=jnp.float32) + b_out).astype(jnp.bfloat16)
        d_norm = jnp.einsum("bsk,hk->bsh", dq_loc, w_flat, preferred_element_type=jnp.float32)
        gg = jnp.sum(d_norm * x_hat, axis=(0, 1))
        gb = jnp.sum(d_norm, axis=(0, 1))
        e = d_norm * ln_gain
        d_ln = inv_std * (e - jnp.mean(e, axis=-1, keepdims=True) - x_hat * jnp.mean(e * x_hat, axis=-1, keepdims=True))
        grad_x = (dy_blk.astype(jnp.float32) + d_ln).astype(jnp.bfloat16)

        gbo = jnp.sum(after(dy_blk, gw).astype(jnp.float32), axis=(0, 1))
        vec = jnp.concatenate([gb_mine, gg, gb, gbo])
        vecs = jnp.stack([vec] + [swap(vec, r) for r in range(1, sp_size)])
        grad_b_qkv = vecs[:, :width][jnp.arange(sp_size) ^ me].reshape(b_qkv.shape)
        sums = jnp.sum(vecs[:, width:], axis=0)
        grad_gain, grad_bias, grad_b_out = sums[:hidden], sums[hidden:2 * hidden], sums[2 * hidden:]

        wo_pieces = gather(gwo)
        grad_w_out = stack_rows(me_arr, wo_pieces).reshape(hidden, hidden)
        grad_w_qkv = None
        group = sp_size // 2
        row = 0
        for n in CHUNKS:
            pieces = gather(gw[row:row + n])
            for far in (0, 1):
                grad_w_qkv = place(me_arr, pieces[far * group:(far + 1) * group], far, row, grad_w_qkv,
                                   (hidden, 3, num_heads, head_dim), heads, head_dim)
            row += n
        grad_w_qkv = jnp.transpose(grad_w_qkv, (0, 2, 1, 3))
        return (y_blk, grad_x, grad_w_qkv, grad_b_qkv, grad_w_out, grad_b_out, grad_gain, grad_bias)

    act_spec = P("dp", "sp", None)
    tok_spec = P("dp", "sp")
    in_specs = (act_spec, tok_spec, tok_spec, P(), P(), P(), P(), P(), P(), act_spec)
    out_specs = (act_spec, act_spec, P("dp", None, None, None), P("dp", None, None), P("dp", None), P("dp"), P("dp"), P("dp"))
    return jax.shard_map(block_fn, mesh=mesh, in_specs=in_specs, out_specs=out_specs, check_vma=False)
```

```python
import functools

import jax
import jax.numpy as jnp
from jax import lax
from jax.experimental import pallas as pl
from jax.experimental.pallas import tpu as pltpu
from jax.sharding import PartitionSpec as P


NORM_EPS = 1e-5
MASK_FILL = -1e30
LOG2E = 1.4426950408889634


NT = (((1,), (1,)), ((), ()))
NN = (((1,), (0,)), ((), ()))


def dot(a, b, dims=NN):
    return lax.dot_general(a, b, dims, preferred_element_type=jnp.float32)


def stage_kernel(me_ref, slope_ref, x0_ref, x1_ref, d0_ref, d1_ref, w_ref, b_ref, wo_ref, pos_ref, *refs, nblk, blk, dim, heads, scale, first):
    if first:
        gwi_ref = gwoi_ref = None
    else:
        gwi_ref, gwoi_ref = refs[:2]
        refs = refs[2:]
    out_ref, gw_ref, gwo_ref, qkv_ref, do_ref, s_ref, dk_ref, dv_ref, kt_ref, vt_ref, ot_ref, xv_ref, dv_all_ref, x_sem, d_sem = refs
    step = pl.program_id(0)
    me = me_ref[0]
    width = 3 * dim
    half = nblk // 2

    def load(b):
        p, at = b // half, pl.ds((b % half) * blk, blk)
        return (pltpu.make_async_copy((x0_ref, x1_ref)[p].at[at], xv_ref.at[b], x_sem.at[b]),
                pltpu.make_async_copy((d0_ref, d1_ref)[p].at[at], dv_all_ref.at[b], d_sem.at[b]))

    @pl.when(step == 0)
    def _():
        for b in range(nblk):
            for copy in load(b):
                copy.start()

    for b in range(nblk):
        @pl.when(step == b)
        def _(b=b):
            for copy in load(b):
                copy.wait()

    @pl.when(step < nblk)
    def _():
        tok = jnp.bitwise_xor(me, 2 * lax.rem(step, half) + lax.div(step, half))
        pair, side = lax.div(tok, 2), lax.rem(tok, 2)
        at = pl.ds(pl.multiple_of(tok * blk, blk), blk)
        qkv = (dot(xv_ref[step], w_ref[...]) + b_ref[...]).astype(jnp.bfloat16)
        qkv_ref[at, :] = qkv
        do_ref[at, :] = dot(dv_all_ref[step], wo_ref[...], NT).astype(jnp.bfloat16)
        for h in range(heads):
            lanes = pl.ds(pl.multiple_of(side * blk, blk), blk)
            kt_ref[h, pair, :, lanes] = qkv[:, h * width + dim:h * width + 2 * dim].T
            vt_ref[h, pair, :, lanes] = qkv[:, h * width + 2 * dim:(h + 1) * width].T

    @pl.when(step == 0)
    def _():
        dk_ref[...] = jnp.zeros_like(dk_ref)
        dv_ref[...] = jnp.zeros_like(dv_ref)

    @pl.when((step >= nblk) & (step < nblk + half))
    def _():
        attend(step - nblk, slope_ref, qkv_ref, do_ref, pos_ref, out_ref, s_ref, dk_ref, dv_ref, kt_ref, vt_ref, ot_ref,
               nblk=nblk, blk=blk, dim=dim, heads=heads, scale=scale)

    @pl.when(step >= nblk + half)
    def _():
        tile = gw_ref.shape[0]
        cols = pl.ds(pl.multiple_of((step - nblk - half) * tile, tile), tile)
        places = []
        for j in range(nblk):
            r = jnp.bitwise_xor(me, j)
            places.append(lax.rem(r, 2) * half + lax.div(r, 2))
        xt = jnp.concatenate([xv_ref[p, :, cols] for p in places], axis=0)
        gw = dot(xt.T, out_ref[:, :heads * width])
        gwo = 0.0
        for j, p in enumerate(places):
            gwo += dot(ot_ref[j // 2, :, (j % 2) * blk:(j % 2 + 1) * blk], dv_all_ref[p, :, cols])
        gw_ref[...] = gw if first else gwi_ref[...] + gw
        gwo_ref[...] = gwo if first else gwoi_ref[...] + gwo


def attend(i, slope_ref, qkv_ref, do_ref, pos_ref, out_ref, s_ref, dk_ref, dv_ref, kt_ref, vt_ref, ot_ref,
           *, nblk, blk, dim, heads, scale):
    width = 3 * dim
    big = 2 * blk

    def rows(m):
        return pl.ds(pl.multiple_of(m * big, big), big)

    def fold(t, op):
        return op(t.reshape(big // 8, 8, big), axis=0)

    qrows = rows(i)
    qs = [qkv_ref[qrows, h * width:h * width + dim] for h in range(heads)]
    dos = [do_ref[qrows, h * dim:(h + 1) * dim] for h in range(heads)]
    dots = [d.T for d in dos]
    pos_first = pos_ref[pl.ds(pl.multiple_of(i * big, big), 8), 0:1][:1]

    def scores(m, h):
        k = qkv_ref[rows(m), h * width + dim:h * width + 2 * dim]
        bias = (pos_ref[rows(m), 0:1] - pos_first) * slope_ref[h] + pos_ref[rows(m), 1:2]
        return dot(k, qs[h], NT) * (scale * LOG2E) + bias

    def score_pair(m, mx, masked):
        new = []
        for h in range(heads):
            s = scores(m, h)
            if masked:
                seen = lax.broadcasted_iota(jnp.int32, (big, big), 0) <= lax.broadcasted_iota(jnp.int32, (big, big), 1)
                s = jnp.where(seen, s, MASK_FILL)
            s_ref[h, m] = s
            new.append(jnp.maximum(mx[h], fold(s, jnp.max)))
        return tuple(new)

    start = tuple(jnp.full((8, big), MASK_FILL, jnp.float32) for _ in range(heads))
    mx = lax.fori_loop(0, i, lambda m, c: score_pair(m, c, False), start)
    mx = score_pair(i, mx, True)
    tops = [jnp.max(v, axis=0, keepdims=True) for v in mx]

    def weigh_pair(m, carry):
        tot, acc = [], []
        for h in range(heads):
            p = jnp.exp2(s_ref[h, m] - tops[h])
            s_ref[h, m] = p
            tot.append(carry[0][h] + fold(p, jnp.sum))
            acc.append(carry[1][h] + dot(vt_ref[h, m], p.astype(jnp.bfloat16)))
        return tuple(tot), tuple(acc)

    zero_t = tuple(jnp.zeros((dim, big), jnp.float32) for _ in range(heads))
    tot, ots = lax.fori_loop(0, i + 1, weigh_pair, (tuple(jnp.zeros((8, big), jnp.float32) for _ in range(heads)), zero_t))
    inv = [1.0 / jnp.sum(t, axis=0, keepdims=True) for t in tot]
    rs = []
    for h in range(heads):
        o_lo = (ots[h] * inv[h]).astype(jnp.bfloat16)
        rs.append(jnp.sum(dots[h].astype(jnp.float32) * o_lo.astype(jnp.float32), axis=0, keepdims=True))
        ot_ref[i, h * dim:(h + 1) * dim, :] = o_lo
        out_ref[qrows, heads * width + h * dim:heads * width + (h + 1) * dim] = o_lo.T

    def grad_pair(m, acc):
        new = []
        for h in range(heads):
            v = qkv_ref[rows(m), h * width + 2 * dim:(h + 1) * width]
            p = s_ref[h, m] * inv[h]
            ds = (p * (dot(v, dos[h], NT) - rs[h])).astype(jnp.bfloat16)
            dv_ref[h, m] += dot(p.astype(jnp.bfloat16), dos[h])
            dk_ref[h, m] += dot(ds, qs[h])
            new.append(acc[h] + dot(kt_ref[h, m], ds))
        return tuple(new)

    dqts = lax.fori_loop(0, i + 1, grad_pair, zero_t)
    for h in range(heads):
        out_ref[qrows, h * width:h * width + dim] = (dqts[h] * scale).astype(jnp.bfloat16).T

    @pl.when(i == nblk // 2 - 1)
    def _():
        for m in range(nblk // 2):
            at = slice(m * big, (m + 1) * big)
            for h in range(heads):
                out_ref[at, h * width + dim:h * width + 2 * dim] = (dk_ref[h, m] * scale).astype(jnp.bfloat16)
                out_ref[at, h * width + 2 * dim:(h + 1) * width] = dv_ref[h, m].astype(jnp.bfloat16)


def stage(me, slopes, x_two, d_two, w, b, wo, pos, gw, gwo, nblk, heads, dim):
    n, hidden = x_two[0].shape
    seq = 2 * n
    blk = seq // nblk
    half = nblk // 2
    width, owidth = 3 * heads * dim, heads * dim
    tile = hidden // nblk
    first = gw is None
    body = functools.partial(stage_kernel, nblk=nblk, blk=blk, dim=dim, heads=heads, scale=dim ** -0.5, first=first)
    tiles = heads * nblk * (nblk + 1) // 2

    def late(i):
        return jnp.maximum(i - nblk - half, 0)

    def fixed(shape):
        return pl.BlockSpec(shape, lambda i, m: (0, 0), pipeline_mode=pl.Buffered(1))

    gw_spec = pl.BlockSpec((tile, width), lambda i, m: (late(i), 0))
    gwo_spec = pl.BlockSpec((owidth, tile), lambda i, m: (0, late(i)))
    args = [x_two[0], x_two[1], d_two[0], d_two[1], w, b, wo, pos]
    in_specs = [pl.BlockSpec(memory_space=pltpu.SMEM)] + [pl.BlockSpec(memory_space=pl.ANY)] * 4 + [
                fixed(w.shape), fixed(b.shape), fixed(wo.shape), fixed(pos.shape)]
    aliases = {}
    if not first:
        args += [gw, gwo]
        in_specs += [gw_spec, gwo_spec]
        aliases = {10: 1, 11: 2}
    flops = tiles * 12 * blk * blk * dim + 4 * seq * hidden * (width + owidth)
    return pl.pallas_call(
        body,
        grid_spec=pltpu.PrefetchScalarGridSpec(
            num_scalar_prefetch=1,
            grid=(2 * nblk + half,),
            in_specs=in_specs,
            out_specs=[pl.BlockSpec((seq, width + owidth), lambda i, m: (0, 0), pipeline_mode=pl.Buffered(1)), gw_spec, gwo_spec],
            scratch_shapes=[
                pltpu.VMEM((seq, width), jnp.bfloat16),
                pltpu.VMEM((seq, owidth), jnp.bfloat16),
                pltpu.VMEM((heads, half, 2 * blk, 2 * blk), jnp.float32),
                pltpu.VMEM((heads, half, 2 * blk, dim), jnp.float32),
                pltpu.VMEM((heads, half, 2 * blk, dim), jnp.float32),
                pltpu.VMEM((heads, half, dim, 2 * blk), jnp.bfloat16),
                pltpu.VMEM((heads, half, dim, 2 * blk), jnp.bfloat16),
                pltpu.VMEM((half, owidth, 2 * blk), jnp.bfloat16),
                pltpu.VMEM((nblk, blk, hidden), jnp.bfloat16),
                pltpu.VMEM((nblk, blk, hidden), jnp.bfloat16),
                pltpu.SemaphoreType.DMA((nblk,)),
                pltpu.SemaphoreType.DMA((nblk,)),
            ],
        ),
        out_shape=[jax.ShapeDtypeStruct((seq, width + owidth), jnp.bfloat16),
                   jax.ShapeDtypeStruct((hidden, width), jnp.float32),
                   jax.ShapeDtypeStruct((owidth, hidden), jnp.float32)],
        input_output_aliases=aliases,
        compiler_params=pltpu.CompilerParams(
            dimension_semantics=("arbitrary",), vmem_limit_bytes=60 * 1024 * 1024),
        cost_estimate=pl.CostEstimate(flops=flops, bytes_accessed=seq * hidden * 8, transcendentals=tiles * blk * blk),
        name="stage",
    )(me, slopes, *args)


def place_kernel(me_ref, p0, p1, p2, p3, *refs, heads, dim, group):
    out_ref = refs[-1]
    pieces = (p0, p1, p2, p3)
    mine = lax.rem(me_ref[0], group)
    for m in range(group):
        @pl.when(mine == m)
        def _(m=m):
            for r in range(group):
                for h in range(heads):
                    for c in range(3):
                        at = (h * 3 + c) * dim
                        out_ref[:, c, (m ^ r) * heads + h, :] = pieces[r][:, at:at + dim]


def place(me, pieces, far, row, full, shape, heads, dim):
    group = len(pieces)
    n, width = pieces[0].shape
    rows = 128
    first = row // rows
    aliases = {}
    args = list(pieces)
    in_specs = [pl.BlockSpec((rows, width), lambda g, m: (g, 0))] * group
    if full is not None:
        in_specs.append(pl.BlockSpec(memory_space=pl.ANY))
        args.append(full)
        aliases = {group + 1: 0}
    return pl.pallas_call(
        functools.partial(place_kernel, heads=heads, dim=dim, group=group),
        grid_spec=pltpu.PrefetchScalarGridSpec(
            num_scalar_prefetch=1,
            grid=(n // rows,),
            in_specs=in_specs,
            out_specs=pl.BlockSpec(
                (rows, 3, group * heads, dim),
                lambda g, m: (first + g, 0, jnp.bitwise_xor(lax.div(m[0], group), far), 0)),
        ),
        out_shape=jax.ShapeDtypeStruct(shape, jnp.float32),
        input_output_aliases=aliases,
        cost_estimate=pl.CostEstimate(flops=group * n * width * 30, bytes_accessed=group * n * width * 8, transcendentals=0),
        name="place",
    )(me, *args)


def stack_kernel(me_ref, *refs):
    out_ref = refs[-1]
    for r, p_ref in enumerate(refs[:-1]):
        out_ref[jnp.bitwise_xor(me_ref[0], r)] = p_ref[...]


def stack_rows(me, pieces):
    n, width = pieces[0].shape
    rows = 32
    return pl.pallas_call(
        stack_kernel,
        grid_spec=pltpu.PrefetchScalarGridSpec(
            num_scalar_prefetch=1,
            grid=(n // rows,),
            in_specs=[pl.BlockSpec((rows, width), lambda g, m: (g, 0))] * len(pieces),
            out_specs=pl.BlockSpec((len(pieces), rows, width), lambda g, m: (0, g, 0)),
        ),
        out_shape=jax.ShapeDtypeStruct((len(pieces), n, width), jnp.float32),
        cost_estimate=pl.CostEstimate(flops=len(pieces) * n * width * 4, bytes_accessed=len(pieces) * n * width * 8, transcendentals=0),
        name="stack_rows",
    )(me, *pieces)


CHUNKS = (640, 640, 512, 256)


def after(value, *others):
    return lax.optimization_barrier((value,) + others)[0]


def solution(mesh):
    sp_size = mesh.shape["sp"]

    def swap(v, r):
        return lax.ppermute(v, "sp", [(i, i ^ r) for i in range(sp_size)])

    def gather(b):
        half = b.shape[0] // 2
        bx, by, bs = swap(b, 2), swap(b, 4), swap(b, 1)
        bd = jnp.concatenate([swap(bx[:half], 4), swap(by[half:], 2)], 0)
        return [b, bs, bx, swap(bx, 1), by, swap(by, 1), bd, swap(bd, 1)]

    def gather_halves(b):
        half = b.shape[0] // 2
        bx, by = swap(b, 2), swap(b, 4)
        mine = jnp.concatenate([b, bx, by, swap(bx[:half], 4), swap(by[half:], 2)], 0)
        return mine, swap(mine, 1)

    def block_fn(x_blk, pos_blk, keep_blk, ln_gain, ln_bias, w_qkv, b_qkv, w_out, b_out, dy_blk):
        batch_loc, seq_loc, hidden = x_blk.shape
        num_heads, head_dim = w_qkv.shape[1], w_qkv.shape[3]
        heads = num_heads // sp_size
        width = heads * 3 * head_dim
        owidth = heads * head_dim
        me = lax.axis_index("sp")
        me_arr = me.reshape(1).astype(jnp.int32)

        def stats(x):
            x_f32 = x.astype(jnp.float32)
            centered = x_f32 - jnp.mean(x_f32, axis=-1, keepdims=True)
            inv_std = lax.rsqrt(jnp.mean(centered * centered, axis=-1, keepdims=True) + NORM_EPS)
            return x_f32, centered * inv_std, inv_std

        def norm(x):
            return (stats(x)[1] * ln_gain + ln_bias).astype(jnp.bfloat16)

        x_norms = [norm(x_blk[s]) for s in range(batch_loc)]

        pk = jnp.stack([pos_blk, keep_blk])
        pk_all = jnp.stack([pk] + [swap(pk, r) for r in range(1, sp_size)])
        pk_all = pk_all[jnp.arange(sp_size) ^ me]
        pk_all = jnp.transpose(pk_all, (1, 2, 0, 3)).reshape(2, batch_loc, sp_size * seq_loc)
        pos_col = jnp.stack([pk_all[0].astype(jnp.float32), jnp.where(pk_all[1] > 0, 0.0, MASK_FILL)], axis=-1)
        head_ids = me * heads + jnp.arange(heads)
        slopes = jnp.exp2(-8.0 * (head_ids + 1).astype(jnp.float32) / num_heads) * LOG2E

        w_flat = after(w_qkv, x_norms[0]).reshape(hidden, sp_size * width)
        w_mine = lax.dynamic_slice_in_dim(w_flat, me * width, width, 1)
        b_mine = lax.dynamic_slice_in_dim(b_qkv.reshape(sp_size, width), me, 1, 0)
        wo_mine = lax.dynamic_slice_in_dim(w_out, me * owidth, owidth, 0)

        gw = gwo = None
        results, parts = [], []
        for s in range(batch_loc):
            x_two = gather_halves(x_norms[s])
            d_two = gather_halves(dy_blk[s])
            res, gw, gwo = stage(me_arr, slopes, x_two, d_two, w_mine, b_mine, wo_mine, pos_col[s], gw, gwo,
                                 sp_size, heads, head_dim)
            blocks = res.reshape(sp_size, seq_loc, width + owidth)
            if s == batch_loc - 2:
                picks = [lax.dynamic_index_in_dim(blocks, me ^ r, 0) for r in range(sp_size)]
                parts.append([swap(v, r) if r else v for r, v in enumerate(picks)])
            else:
                parts.append(lax.all_to_all(blocks, "sp", 0, 0, tiled=True))
            results.append(res)
        gb_mine = sum(jnp.sum(after(d, gw)[:, :width].astype(jnp.float32), axis=0) for d in results)

        got = list(lax.optimization_barrier((parts, gw))[0])
        joined = jnp.zeros((sp_size, seq_loc, width + owidth), jnp.bfloat16)
        for r, v in enumerate(got[batch_loc - 2]):
            joined = lax.dynamic_update_slice(joined, v, (me ^ r, 0, 0))
        got[batch_loc - 2] = joined
        got = jnp.stack(got)
        got = jnp.transpose(got, (0, 2, 1, 3))
        dq_loc = got[..., :width].reshape(batch_loc, seq_loc, sp_size * width)
        o_loc = got[..., width:].reshape(batch_loc, seq_loc, hidden)
        x_f32, x_hat, inv_std = stats(after(x_blk, gw))
        y_blk = (x_f32 + jnp.einsum("bsh,hk->bsk", o_loc, w_out, preferred_element_type=jnp.float32) + b_out).astype(jnp.bfloat16)
        d_norm = jnp.einsum("bsk,hk->bsh", dq_loc, w_flat, preferred_element_type=jnp.float32)
        gg = jnp.sum(d_norm * x_hat, axis=(0, 1))
        gb = jnp.sum(d_norm, axis=(0, 1))
        e = d_norm * ln_gain
        d_ln = inv_std * (e - jnp.mean(e, axis=-1, keepdims=True) - x_hat * jnp.mean(e * x_hat, axis=-1, keepdims=True))
        grad_x = (dy_blk.astype(jnp.float32) + d_ln).astype(jnp.bfloat16)

        gbo = jnp.sum(after(dy_blk, gw).astype(jnp.float32), axis=(0, 1))
        vec = jnp.concatenate([gb_mine, gg, gb, gbo])
        vecs = jnp.stack([vec] + [swap(vec, r) for r in range(1, sp_size)])
        grad_b_qkv = vecs[:, :width][jnp.arange(sp_size) ^ me].reshape(b_qkv.shape)
        sums = jnp.sum(vecs[:, width:], axis=0)
        grad_gain, grad_bias, grad_b_out = sums[:hidden], sums[hidden:2 * hidden], sums[2 * hidden:]

        wo_pieces = gather(gwo)
        grad_w_out = stack_rows(me_arr, wo_pieces).reshape(hidden, hidden)
        grad_w_qkv = None
        group = sp_size // 2
        row = 0
        for n in CHUNKS:
            pieces = gather(gw[row:row + n])
            for far in (0, 1):
                grad_w_qkv = place(me_arr, pieces[far * group:(far + 1) * group], far, row, grad_w_qkv,
                                   (hidden, 3, num_heads, head_dim), heads, head_dim)
            row += n
        grad_w_qkv = jnp.transpose(grad_w_qkv, (0, 2, 1, 3))
        return (y_blk, grad_x, grad_w_qkv, grad_b_qkv, grad_w_out, grad_b_out, grad_gain, grad_bias)

    act_spec = P("dp", "sp", None)
    tok_spec = P("dp", "sp")
    in_specs = (act_spec, tok_spec, tok_spec, P(), P(), P(), P(), P(), P(), act_spec)
    out_specs = (act_spec, act_spec, P("dp", None, None, None), P("dp", None, None), P("dp", None), P("dp"), P("dp"), P("dp"))
    return jax.shard_map(block_fn, mesh=mesh, in_specs=in_specs, out_specs=out_specs, check_vma=False)
```

```python
import functools

import jax
import jax.numpy as jnp
from jax import lax
from jax.experimental import pallas as pl
from jax.experimental.pallas import tpu as pltpu
from jax.sharding import PartitionSpec as P


NORM_EPS = 1e-5
MASK_FILL = -1e30
LOG2E = 1.4426950408889634


NT = (((1,), (1,)), ((), ()))
NN = (((1,), (0,)), ((), ()))


def dot(a, b, dims=NN):
    return lax.dot_general(a, b, dims, preferred_element_type=jnp.float32)


def stage_kernel(me_ref, slope_ref, w_ref, b_ref, wo_ref, pos_ref, *refs, nblk, blk, dim, heads, scale, first):
    count = nblk + 2
    x_pieces, d_pieces, refs = refs[:count], refs[count:2 * count], refs[2 * count:]
    if first:
        gwi_ref = gwoi_ref = None
    else:
        gwi_ref, gwoi_ref = refs[:2]
        refs = refs[2:]
    out_ref, gw_ref, gwo_ref, qkv_ref, do_ref, s_ref, dk_ref, dv_ref, kt_ref, vt_ref, ot_ref, xv_ref, dv_all_ref, x_sem, d_sem = refs
    step = pl.program_id(0)
    me = me_ref[0]
    width = 3 * dim
    half = nblk // 2

    def load(b):
        p, q = b // half, b % half
        copies = []
        for pieces, dst, sem in ((x_pieces, xv_ref, x_sem), (d_pieces, dv_all_ref, d_sem)):
            base = p * (half + 1)
            if q < half - 1:
                copies.append(pltpu.make_async_copy(pieces[base + q], dst.at[b], sem.at[b]))
            else:
                for e in range(2):
                    at = pl.ds(e * (blk // 2), blk // 2)
                    copies.append(pltpu.make_async_copy(pieces[base + q + e], dst.at[b, at], sem.at[b if e == 0 else nblk + p]))
        return copies

    @pl.when(step == 0)
    def _():
        for b in range(nblk):
            for copy in load(b):
                copy.start()

    for b in range(nblk):
        @pl.when(step == b)
        def _(b=b):
            for copy in load(b):
                copy.wait()

    @pl.when(step < nblk)
    def _():
        tok = jnp.bitwise_xor(me, 2 * lax.rem(step, half) + lax.div(step, half))
        pair, side = lax.div(tok, 2), lax.rem(tok, 2)
        at = pl.ds(pl.multiple_of(tok * blk, blk), blk)
        qkv = (dot(xv_ref[step], w_ref[...]) + b_ref[...]).astype(jnp.bfloat16)
        qkv_ref[at, :] = qkv
        do_ref[at, :] = dot(dv_all_ref[step], wo_ref[...], NT).astype(jnp.bfloat16)
        for h in range(heads):
            lanes = pl.ds(pl.multiple_of(side * blk, blk), blk)
            kt_ref[h, pair, :, lanes] = qkv[:, h * width + dim:h * width + 2 * dim].T
            vt_ref[h, pair, :, lanes] = qkv[:, h * width + 2 * dim:(h + 1) * width].T

    @pl.when(step == 0)
    def _():
        dk_ref[...] = jnp.zeros_like(dk_ref)
        dv_ref[...] = jnp.zeros_like(dv_ref)

    @pl.when((step >= nblk) & (step < nblk + half))
    def _():
        attend(step - nblk, slope_ref, qkv_ref, do_ref, pos_ref, out_ref, s_ref, dk_ref, dv_ref, kt_ref, vt_ref, ot_ref,
               nblk=nblk, blk=blk, dim=dim, heads=heads, scale=scale)

    @pl.when(step >= nblk + half)
    def _():
        tile = gw_ref.shape[0]
        cols = pl.ds(pl.multiple_of((step - nblk - half) * tile, tile), tile)
        places = []
        for j in range(nblk):
            r = jnp.bitwise_xor(me, j)
            places.append(lax.rem(r, 2) * half + lax.div(r, 2))
        xt = jnp.concatenate([xv_ref[p, :, cols] for p in places], axis=0)
        gw = dot(xt.T, out_ref[:, :heads * width])
        gwo = 0.0
        for j, p in enumerate(places):
            gwo += dot(ot_ref[j // 2, :, (j % 2) * blk:(j % 2 + 1) * blk], dv_all_ref[p, :, cols])
        gw_ref[...] = gw if first else gwi_ref[...] + gw
        gwo_ref[...] = gwo if first else gwoi_ref[...] + gwo


def attend(i, slope_ref, qkv_ref, do_ref, pos_ref, out_ref, s_ref, dk_ref, dv_ref, kt_ref, vt_ref, ot_ref,
           *, nblk, blk, dim, heads, scale):
    width = 3 * dim
    big = 2 * blk

    def rows(m):
        return pl.ds(pl.multiple_of(m * big, big), big)

    def fold(t, op):
        return op(t.reshape(big // 8, 8, big), axis=0)

    qrows = rows(i)
    qs = [qkv_ref[qrows, h * width:h * width + dim] for h in range(heads)]
    dos = [do_ref[qrows, h * dim:(h + 1) * dim] for h in range(heads)]
    dots = [d.T for d in dos]
    pos_first = pos_ref[pl.ds(pl.multiple_of(i * big, big), 8), 0:1][:1]

    def scores(m, h):
        k = qkv_ref[rows(m), h * width + dim:h * width + 2 * dim]
        bias = (pos_ref[rows(m), 0:1] - pos_first) * slope_ref[h] + pos_ref[rows(m), 1:2]
        return dot(k, qs[h], NT) * (scale * LOG2E) + bias

    def score_pair(m, mx, masked):
        new = []
        for h in range(heads):
            s = scores(m, h)
            if masked:
                seen = lax.broadcasted_iota(jnp.int32, (big, big), 0) <= lax.broadcasted_iota(jnp.int32, (big, big), 1)
                s = jnp.where(seen, s, MASK_FILL)
            s_ref[h, m] = s
            new.append(jnp.maximum(mx[h], fold(s, jnp.max)))
        return tuple(new)

    start = tuple(jnp.full((8, big), MASK_FILL, jnp.float32) for _ in range(heads))
    mx = lax.fori_loop(0, i, lambda m, c: score_pair(m, c, False), start)
    mx = score_pair(i, mx, True)
    tops = [jnp.max(v, axis=0, keepdims=True) for v in mx]

    def weigh_pair(m, carry):
        tot, acc = [], []
        for h in range(heads):
            p = jnp.exp2(s_ref[h, m] - tops[h])
            s_ref[h, m] = p
            tot.append(carry[0][h] + fold(p, jnp.sum))
            acc.append(carry[1][h] + dot(vt_ref[h, m], p.astype(jnp.bfloat16)))
        return tuple(tot), tuple(acc)

    zero_t = tuple(jnp.zeros((dim, big), jnp.float32) for _ in range(heads))
    tot, ots = lax.fori_loop(0, i + 1, weigh_pair, (tuple(jnp.zeros((8, big), jnp.float32) for _ in range(heads)), zero_t))
    inv = [1.0 / jnp.sum(t, axis=0, keepdims=True) for t in tot]
    rs = []
    for h in range(heads):
        o_lo = (ots[h] * inv[h]).astype(jnp.bfloat16)
        rs.append(jnp.sum(dots[h].astype(jnp.float32) * o_lo.astype(jnp.float32), axis=0, keepdims=True))
        ot_ref[i, h * dim:(h + 1) * dim, :] = o_lo
        out_ref[qrows, heads * width + h * dim:heads * width + (h + 1) * dim] = o_lo.T

    def grad_pair(m, acc):
        new = []
        for h in range(heads):
            v = qkv_ref[rows(m), h * width + 2 * dim:(h + 1) * width]
            p = s_ref[h, m] * inv[h]
            ds = (p * (dot(v, dos[h], NT) - rs[h])).astype(jnp.bfloat16)
            dv_ref[h, m] += dot(p.astype(jnp.bfloat16), dos[h])
            dk_ref[h, m] += dot(ds, qs[h])
            new.append(acc[h] + dot(kt_ref[h, m], ds))
        return tuple(new)

    dqts = lax.fori_loop(0, i + 1, grad_pair, zero_t)
    for h in range(heads):
        out_ref[qrows, h * width:h * width + dim] = (dqts[h] * scale).astype(jnp.bfloat16).T

    @pl.when(i == nblk // 2 - 1)
    def _():
        for m in range(nblk // 2):
            at = slice(m * big, (m + 1) * big)
            for h in range(heads):
                out_ref[at, h * width + dim:h * width + 2 * dim] = (dk_ref[h, m] * scale).astype(jnp.bfloat16)
                out_ref[at, h * width + 2 * dim:(h + 1) * width] = dv_ref[h, m].astype(jnp.bfloat16)


def stage(me, slopes, x_two, d_two, w, b, wo, pos, gw, gwo, nblk, heads, dim):
    blk, hidden = x_two[0].shape
    seq = nblk * blk
    half = nblk // 2
    width, owidth = 3 * heads * dim, heads * dim
    tile = hidden // nblk
    first = gw is None
    body = functools.partial(stage_kernel, nblk=nblk, blk=blk, dim=dim, heads=heads, scale=dim ** -0.5, first=first)
    tiles = heads * nblk * (nblk + 1) // 2

    def late(i):
        return jnp.maximum(i - nblk - half, 0)

    def fixed(shape):
        return pl.BlockSpec(shape, lambda i, m: (0, 0), pipeline_mode=pl.Buffered(1))

    gw_spec = pl.BlockSpec((tile, width), lambda i, m: (late(i), 0))
    gwo_spec = pl.BlockSpec((owidth, tile), lambda i, m: (0, late(i)))
    args = [w, b, wo, pos, *x_two, *d_two]
    in_specs = [pl.BlockSpec(memory_space=pltpu.SMEM), fixed(w.shape), fixed(b.shape), fixed(wo.shape), fixed(pos.shape)]
    in_specs += [pl.BlockSpec(memory_space=pl.ANY)] * (2 * (nblk + 2))
    aliases = {}
    if not first:
        aliases = {len(args) + 2: 1, len(args) + 3: 2}
        args += [gw, gwo]
        in_specs += [gw_spec, gwo_spec]
    flops = tiles * 12 * blk * blk * dim + 4 * seq * hidden * (width + owidth)
    return pl.pallas_call(
        body,
        grid_spec=pltpu.PrefetchScalarGridSpec(
            num_scalar_prefetch=1,
            grid=(2 * nblk + half,),
            in_specs=in_specs,
            out_specs=[pl.BlockSpec((seq, width + owidth), lambda i, m: (0, 0), pipeline_mode=pl.Buffered(1)), gw_spec, gwo_spec],
            scratch_shapes=[
                pltpu.VMEM((seq, width), jnp.bfloat16),
                pltpu.VMEM((seq, owidth), jnp.bfloat16),
                pltpu.VMEM((heads, half, 2 * blk, 2 * blk), jnp.float32),
                pltpu.VMEM((heads, half, 2 * blk, dim), jnp.float32),
                pltpu.VMEM((heads, half, 2 * blk, dim), jnp.float32),
                pltpu.VMEM((heads, half, dim, 2 * blk), jnp.bfloat16),
                pltpu.VMEM((heads, half, dim, 2 * blk), jnp.bfloat16),
                pltpu.VMEM((half, owidth, 2 * blk), jnp.bfloat16),
                pltpu.VMEM((nblk, blk, hidden), jnp.bfloat16),
                pltpu.VMEM((nblk, blk, hidden), jnp.bfloat16),
                pltpu.SemaphoreType.DMA((nblk + 2,)),
                pltpu.SemaphoreType.DMA((nblk + 2,)),
            ],
        ),
        out_shape=[jax.ShapeDtypeStruct((seq, width + owidth), jnp.bfloat16),
                   jax.ShapeDtypeStruct((hidden, width), jnp.float32),
                   jax.ShapeDtypeStruct((owidth, hidden), jnp.float32)],
        input_output_aliases=aliases,
        compiler_params=pltpu.CompilerParams(
            dimension_semantics=("arbitrary",), vmem_limit_bytes=60 * 1024 * 1024),
        cost_estimate=pl.CostEstimate(flops=flops, bytes_accessed=seq * hidden * 8, transcendentals=tiles * blk * blk),
        name="stage",
    )(me, slopes, *args)


def place_kernel(me_ref, p0, p1, p2, p3, *refs, heads, dim, group):
    out_ref = refs[-1]
    pieces = (p0, p1, p2, p3)
    mine = lax.rem(me_ref[0], group)
    for m in range(group):
        @pl.when(mine == m)
        def _(m=m):
            for r in range(group):
                for h in range(heads):
                    for c in range(3):
                        at = (h * 3 + c) * dim
                        out_ref[:, c, (m ^ r) * heads + h, :] = pieces[r][:, at:at + dim]


def place(me, pieces, far, row, full, shape, heads, dim):
    group = len(pieces)
    n, width = pieces[0].shape
    rows = 128
    first = row // rows
    aliases = {}
    args = list(pieces)
    in_specs = [pl.BlockSpec((rows, width), lambda g, m: (g, 0))] * group
    if full is not None:
        in_specs.append(pl.BlockSpec(memory_space=pl.ANY))
        args.append(full)
        aliases = {group + 1: 0}
    return pl.pallas_call(
        functools.partial(place_kernel, heads=heads, dim=dim, group=group),
        grid_spec=pltpu.PrefetchScalarGridSpec(
            num_scalar_prefetch=1,
            grid=(n // rows,),
            in_specs=in_specs,
            out_specs=pl.BlockSpec(
                (rows, 3, group * heads, dim),
                lambda g, m: (first + g, 0, jnp.bitwise_xor(lax.div(m[0], group), far), 0)),
        ),
        out_shape=jax.ShapeDtypeStruct(shape, jnp.float32),
        input_output_aliases=aliases,
        cost_estimate=pl.CostEstimate(flops=group * n * width * 30, bytes_accessed=group * n * width * 8, transcendentals=0),
        name="place",
    )(me, *args)


def stack_kernel(me_ref, *refs):
    out_ref = refs[-1]
    for r, p_ref in enumerate(refs[:-1]):
        out_ref[jnp.bitwise_xor(me_ref[0], r)] = p_ref[...]


def stack_rows(me, pieces):
    n, width = pieces[0].shape
    rows = 32
    return pl.pallas_call(
        stack_kernel,
        grid_spec=pltpu.PrefetchScalarGridSpec(
            num_scalar_prefetch=1,
            grid=(n // rows,),
            in_specs=[pl.BlockSpec((rows, width), lambda g, m: (g, 0))] * len(pieces),
            out_specs=pl.BlockSpec((len(pieces), rows, width), lambda g, m: (0, g, 0)),
        ),
        out_shape=jax.ShapeDtypeStruct((len(pieces), n, width), jnp.float32),
        cost_estimate=pl.CostEstimate(flops=len(pieces) * n * width * 4, bytes_accessed=len(pieces) * n * width * 8, transcendentals=0),
        name="stack_rows",
    )(me, *pieces)


CHUNKS = (768, 640, 384, 256)


def after(value, *others):
    return lax.optimization_barrier((value,) + others)[0]


def solution(mesh):
    sp_size = mesh.shape["sp"]

    def swap(v, r):
        return lax.ppermute(v, "sp", [(i, i ^ r) for i in range(sp_size)])

    def gather(b):
        half = b.shape[0] // 2
        bx, by, bs = swap(b, 2), swap(b, 4), swap(b, 1)
        bd = jnp.concatenate([swap(bx[:half], 4), swap(by[half:], 2)], 0)
        return [b, bs, bx, swap(bx, 1), by, swap(by, 1), bd, swap(bd, 1)]

    def gather_pieces(b):
        half = b.shape[0] // 2
        bx, by, bs = swap(b, 2), swap(b, 4), swap(b, 1)
        d1, d2 = swap(bx[:half], 4), swap(by[half:], 2)
        return [b, bx, by, d1, d2, bs, swap(bx, 1), swap(by, 1), swap(d1, 1), swap(d2, 1)]

    def block_fn(x_blk, pos_blk, keep_blk, ln_gain, ln_bias, w_qkv, b_qkv, w_out, b_out, dy_blk):
        batch_loc, seq_loc, hidden = x_blk.shape
        num_heads, head_dim = w_qkv.shape[1], w_qkv.shape[3]
        heads = num_heads // sp_size
        width = heads * 3 * head_dim
        owidth = heads * head_dim
        me = lax.axis_index("sp")
        me_arr = me.reshape(1).astype(jnp.int32)

        def stats(x):
            x_f32 = x.astype(jnp.float32)
            centered = x_f32 - jnp.mean(x_f32, axis=-1, keepdims=True)
            inv_std = lax.rsqrt(jnp.mean(centered * centered, axis=-1, keepdims=True) + NORM_EPS)
            return x_f32, centered * inv_std, inv_std

        def norm(x):
            return (stats(x)[1] * ln_gain + ln_bias).astype(jnp.bfloat16)

        x_norms = [norm(x_blk[s]) for s in range(batch_loc)]

        pk = jnp.stack([pos_blk, keep_blk])
        pk_all = jnp.stack([pk] + [swap(pk, r) for r in range(1, sp_size)])
        pk_all = pk_all[jnp.arange(sp_size) ^ me]
        pk_all = jnp.transpose(pk_all, (1, 2, 0, 3)).reshape(2, batch_loc, sp_size * seq_loc)
        pos_col = jnp.stack([pk_all[0].astype(jnp.float32), jnp.where(pk_all[1] > 0, 0.0, MASK_FILL)], axis=-1)
        head_ids = me * heads + jnp.arange(heads)
        slopes = jnp.exp2(-8.0 * (head_ids + 1).astype(jnp.float32) / num_heads) * LOG2E

        w_flat = after(w_qkv, x_norms[0]).reshape(hidden, sp_size * width)
        w_mine = lax.dynamic_slice_in_dim(w_flat, me * width, width, 1)
        b_mine = lax.dynamic_slice_in_dim(b_qkv.reshape(sp_size, width), me, 1, 0)
        wo_mine = lax.dynamic_slice_in_dim(w_out, me * owidth, owidth, 0)

        gw = gwo = None
        results, parts = [], []
        for s in range(batch_loc):
            x_two = gather_pieces(x_norms[s])
            d_two = gather_pieces(dy_blk[s])
            res, gw, gwo = stage(me_arr, slopes, x_two, d_two, w_mine, b_mine, wo_mine, pos_col[s], gw, gwo,
                                 sp_size, heads, head_dim)
            blocks = res.reshape(sp_size, seq_loc, width + owidth)
            if s == batch_loc - 2:
                picks = [lax.dynamic_index_in_dim(blocks, me ^ r, 0) for r in range(sp_size)]
                parts.append([swap(v, r) if r else v for r, v in enumerate(picks)])
            else:
                parts.append(lax.all_to_all(blocks, "sp", 0, 0, tiled=True))
            results.append(res)
        gb_mine = sum(jnp.sum(after(d, gw)[:, :width].astype(jnp.float32), axis=0) for d in results)

        got = list(lax.optimization_barrier((parts, gw))[0])
        joined = jnp.zeros((sp_size, seq_loc, width + owidth), jnp.bfloat16)
        for r, v in enumerate(got[batch_loc - 2]):
            joined = lax.dynamic_update_slice(joined, v, (me ^ r, 0, 0))
        got[batch_loc - 2] = joined
        got = jnp.stack(got)
        got = jnp.transpose(got, (0, 2, 1, 3))
        dq_loc = got[..., :width].reshape(batch_loc, seq_loc, sp_size * width)
        o_loc = got[..., width:].reshape(batch_loc, seq_loc, hidden)
        x_f32, x_hat, inv_std = stats(after(x_blk, gw))
        y_blk = (x_f32 + jnp.einsum("bsh,hk->bsk", o_loc, w_out, preferred_element_type=jnp.float32) + b_out).astype(jnp.bfloat16)
        d_norm = jnp.einsum("bsk,hk->bsh", dq_loc, w_flat, preferred_element_type=jnp.float32)
        gg = jnp.sum(d_norm * x_hat, axis=(0, 1))
        gb = jnp.sum(d_norm, axis=(0, 1))
        e = d_norm * ln_gain
        d_ln = inv_std * (e - jnp.mean(e, axis=-1, keepdims=True) - x_hat * jnp.mean(e * x_hat, axis=-1, keepdims=True))
        grad_x = (dy_blk.astype(jnp.float32) + d_ln).astype(jnp.bfloat16)

        gbo = jnp.sum(after(dy_blk, gw).astype(jnp.float32), axis=(0, 1))
        vec = jnp.concatenate([gb_mine, gg, gb, gbo])
        vecs = jnp.stack([vec] + [swap(vec, r) for r in range(1, sp_size)])
        grad_b_qkv = vecs[:, :width][jnp.arange(sp_size) ^ me].reshape(b_qkv.shape)
        sums = jnp.sum(vecs[:, width:], axis=0)
        grad_gain, grad_bias, grad_b_out = sums[:hidden], sums[hidden:2 * hidden], sums[2 * hidden:]

        wo_pieces = gather(gwo)
        grad_w_out = stack_rows(me_arr, wo_pieces).reshape(hidden, hidden)
        grad_w_qkv = None
        group = sp_size // 2
        row = 0
        for g, n in enumerate(CHUNKS):
            pieces = gather(gw[row:row + n])
            if g == 1:
                pieces[0], grad_b_qkv, grad_gain, grad_bias, grad_b_out = lax.optimization_barrier(
                    (pieces[0], grad_b_qkv, grad_gain, grad_bias, grad_b_out))
            for far in (0, 1):
                grad_w_qkv = place(me_arr, pieces[far * group:(far + 1) * group], far, row, grad_w_qkv,
                                   (hidden, 3, num_heads, head_dim), heads, head_dim)
            row += n
        grad_w_qkv = jnp.transpose(grad_w_qkv, (0, 2, 1, 3))
        return (y_blk, grad_x, grad_w_qkv, grad_b_qkv, grad_w_out, grad_b_out, grad_gain, grad_bias)

    act_spec = P("dp", "sp", None)
    tok_spec = P("dp", "sp")
    in_specs = (act_spec, tok_spec, tok_spec, P(), P(), P(), P(), P(), P(), act_spec)
    out_specs = (act_spec, act_spec, P("dp", None, None, None), P("dp", None, None), P("dp", None), P("dp"), P("dp"), P("dp"))
    return jax.shard_map(block_fn, mesh=mesh, in_specs=in_specs, out_specs=out_specs, check_vma=False)
```
